32 devices in a mesh: groups: 2 (over y), ctx: 8 (over z, x), head: 2 (over core).
Axes of the slice: x: 2, y: 2, z: 4, core: 2. Of those that a mesh axis runs over, the one named last changes fastest.
Arguments:
- keys_values: bfloat16 [2, 8192, 1024], P(None, ('groups', 'ctx'), 'head'), parts along dimension 1, may hold values from -6 to 6
- span_order: int32 [32], P('groups'), parts along dimension 0, may hold values from 0 to 15, as said below
- page_table: int32 [64], P('groups'), parts along dimension 0, may hold values from 0 to 31, as said below
Outputs:
- paged_cache: bfloat16 [2, 64, 128, 1024], P(None, ('groups', 'ctx', 'head')), parts along dimension 1
The draws below stay inside these ranges and needn't reach their ends.
There are 2 independent parts, one for each index of `groups`. The reference program is written for one: setup_inputs(seed, part) draws one part's arguments, and reference() takes and returns one part's arrays. A program takes and returns all parts, laid end to end along the dimension named above; each array names one. Nothing has to cross between parts.
Inputs may be any that keep to these rules, and one draw needn't show every extreme that they name: `span_order`: blocks 2 c and 2 c + 1 hold two spans whose numbers add to 15; every span is held once. A permutation of the slots in which page p goes to a slot of p // 2, that is page_table[p] // 2 == p // 2.
All inputs are finite; a program needn't handle non-finite values.
Results may differ from the reference program's by a relative error of at most 0.001.
Values may be sent and summed in bfloat16 or wider, within the bound.
A program may use at most 64 MiB of HBM per device.

```python
import jax
import jax.numpy as jnp

KVH = 8
HD = 128
PAGE = 128
SPAN = 256
SPANS = 16
TOKENS = 4096
PAGES = 32
PAGES_SHARD = 2


def draw_span_order(key, part):
    halves = SPANS // 2
    lower = jax.random.permutation(jax.random.fold_in(key, 11), halves).astype(jnp.int32)
    flipped = jax.random.randint(jax.random.fold_in(key, 12), (halves,), 0, 2)
    first = jnp.where(flipped == 1, SPANS - 1 - lower, lower)
    second = SPANS - 1 - first
    return jnp.stack([first, second], axis=1).reshape(SPANS).astype(jnp.int32)


def draw_page_table(key, part):
    shards = PAGES // PAGES_SHARD
    ranks = jax.random.randint(jax.random.fold_in(key, 21), (shards, PAGES_SHARD), 0, 1048576)
    ranks = ranks * PAGES_SHARD + jnp.arange(PAGES_SHARD, dtype=jnp.int32)[None, :]
    local_slots = jnp.argsort(ranks, axis=1).astype(jnp.int32)
    table = local_slots + jnp.arange(shards, dtype=jnp.int32)[:, None] * PAGES_SHARD
    return table.reshape(PAGES).astype(jnp.int32)


def block_levels(key, extent, pieces, least, high):
    gain = 1.0
    for dim, blocks in pieces:
        draws = jax.random.uniform(jax.random.fold_in(jax.random.fold_in(key, 6), dim), (blocks,), jnp.float32, least / len(pieces), high / len(pieces))
        gain = gain * jnp.repeat(jnp.exp(draws), extent[dim] // blocks).reshape((-1,) + (1,) * (len(extent) - 1 - dim))
    return gain


def gaussian(stream_key, dims, scale, reach, split=(), kind=jnp.bfloat16):
    level = block_levels(stream_key, dims, split, -0.22, 0.18) if split else 1.0
    drawn = jax.random.normal(stream_key, dims, jnp.float32) * scale * level
    return jnp.minimum(jnp.maximum(drawn, -reach), reach).astype(kind)


def setup_inputs(seed: int = 0, part: int = 0) -> dict:
    key_list = jax.random.split(jax.random.key(seed), 4)
    part_keys = jax.random.split(jax.random.fold_in(key_list[3], part), 4)
    return {
        "keys_values": gaussian(part_keys[0], (2, TOKENS, KVH * HD), 1.0, 6.0, ((1, 8), (2, 2))),
        "span_order": draw_span_order(jax.random.fold_in(jax.random.fold_in(key_list[3], part), 71), part),
        "page_table": draw_page_table(jax.random.fold_in(jax.random.fold_in(key_list[3], part), 71), part),
    }


def reference(keys_values, span_order, page_table):
    blocks = keys_values.reshape(2, SPANS, SPAN, KVH * HD)
    context = jnp.zeros_like(blocks).at[:, span_order].set(blocks)
    page_rows = context.reshape(2, PAGES, PAGE, KVH * HD)
    paged_cache = jnp.zeros_like(page_rows).at[:, page_table].set(page_rows)
    return paged_cache
```

```python
import functools

import jax
import jax.numpy as jnp
from jax import lax
from jax.experimental import pallas as pl
from jax.experimental.pallas import tpu as pltpu
from jax.sharding import PartitionSpec as P

PAGE = 128
UNIT = 8
LANES = 128
COL_CHUNKS = 1
INNER_EVERY = 0
MESH = pl.DeviceIdType.MESH


class Chunk:
    def __init__(self, kv, unit, units, col, width, full_width, takers):
        self.kv, self.unit, self.units, self.col, self.width = kv, unit, units, col, width
        self.takers = takers
        self.row_blocks = min(takers, units)
        self.share_units = units // self.row_blocks
        self.col_blocks = takers // self.row_blocks
        self.share_width = width // self.col_blocks
        self.parts = 1 if self.share_width == full_width else 2


def plan(n2, width):
    page_units = PAGE // UNIT
    units = min(page_units, n2)
    col_chunks = max(1, min(COL_CHUNKS, width // (n2 // units * LANES)))
    chunk_width = width // col_chunks
    chunks = []
    for kv in range(2):
        for unit in range(0, page_units, units):
            for col in range(0, width, chunk_width):
                inner = INNER_EVERY and len(chunks) % INNER_EVERY == 0
                takers = n2 // 2 if inner else n2
                chunks.append(Chunk(kv, unit, units, col, chunk_width, width, takers))
    return chunks


def grid(n2):
    grid_rows = n2 // 2
    reach = max(1, grid_rows // 4)
    return grid_rows, reach, -(-(grid_rows - 1) // reach) + 1


def kernel(n2, pages, width, x_ref, order_ref, table_ref, out_ref, *scratch):
    chunks = plan(n2, width)
    count = len(chunks)
    stored = scratch[0:count]
    halves = scratch[count : 2 * count]
    shares = scratch[2 * count : 3 * count]
    routed = scratch[3 * count : 4 * count]
    holder, source_page, load_sem, send1, recv1, send2, recv2, hops = scratch[4 * count :]

    group = lax.axis_index("groups")
    ctx = lax.axis_index("ctx")
    head = lax.axis_index("head")
    me = ctx * 2 + head
    my_half = me // n2
    my_place = lax.rem(me, n2)

    def device(j):
        return (group, j // 2, lax.rem(j, 2))

    def load(k):
        c = chunks[k]
        return pltpu.make_async_copy(
            x_ref.at[c.kv, :, :, pl.ds(c.unit, c.units), :, pl.ds(c.col, c.width)],
            stored[k],
            load_sem.at[k],
        )

    for k in range(count):
        load(k).start()

    barrier = pltpu.get_barrier_semaphore()

    grid_rows, reach, stages = grid(n2)
    row, col = ctx // 2, lax.rem(ctx, 2)
    other = ctx + 1 - 2 * col
    neighbours = 3 + 2 * (jnp.minimum(row, reach) + jnp.minimum(grid_rows - 1 - row, reach))

    def greet(stage):
        sem = barrier if stage == 1 else hops.at[stage]

        def signal(to_ctx, to_head):
            pl.semaphore_signal(
                sem, inc=1, device_id=(group, to_ctx, to_head), device_id_type=MESH
            )

        for step in range(1, reach + 1):
            for sign in (-1, 1):
                to_row = row + sign * step

                @pl.when(jnp.logical_and(to_row >= 0, to_row < grid_rows))
                def _(step=sign * step):
                    for h in range(2):
                        signal(ctx + 2 * step, h)

        signal(ctx, 1 - head)
        for h in range(2):
            signal(other, h)

    def greeted(stage):
        pl.semaphore_wait(barrier if stage == 1 else hops.at[stage], neighbours)

    greet(1)

    first_is_upper = (order_ref[2 * ctx] >= n2).astype(jnp.int32)
    for k in range(count):
        load(k).wait()
        for half in range(2):
            block = first_is_upper if half == 0 else 1 - first_is_upper
            c = chunks[k]
            for share in range(c.takers):
                unit = share // c.col_blocks * c.share_units
                col = share % c.col_blocks * c.share_width
                for page in range(pages):
                    halves[k][half, share, page] = stored[k][
                        block, page, unit : unit + c.share_units, :, col : col + c.share_width
                    ]

    def base(k, half):
        return (n2 - chunks[k].takers) * (1 - half)

    def taking(k):
        share = my_place - base(k, my_half)
        return jnp.logical_and(share >= 0, share < chunks[k].takers)

    def spread(k, half, share):
        return halves[k].at[half, share], shares[k].at[ctx, head]

    def sends(k, d):
        takers = chunks[k].takers
        half = lax.rem(my_half + 1 + d // takers, 2)
        share = lax.rem(me + d, takers)
        return half, share, half * n2 + base(k, half) + share

    def send(k, to_ctx, to_head):
        j = to_ctx * 2 + to_head
        half = j // n2
        share = lax.rem(j, n2) - base(k, half)

        def start():
            src, dst = spread(k, half, share)
            pltpu.make_async_remote_copy(
                src_ref=src,
                dst_ref=dst,
                send_sem=send1.at[k, j],
                recv_sem=recv1.at[k],
                device_id=(group, to_ctx, to_head),
                device_id_type=MESH,
            ).start()

        if chunks[k].takers == n2:
            start()
        else:
            pl.when(jnp.logical_and(share >= 0, share < chunks[k].takers))(start)

    def send_stage(k, stage):
        for step in range(1 - grid_rows, grid_rows):
            for cross in range(2):
                if max(1, -(-abs(step) // reach) + cross) != stage:
                    continue
                to_ctx = (other if cross else ctx) + 2 * step
                if step == 0 and not cross:
                    send(k, ctx, 1 - head)

                    @pl.when(taking(k))
                    def _():
                        src, dst = spread(k, my_half, my_place - base(k, my_half))
                        pltpu.make_async_copy(src, dst, recv1.at[k]).start()

                else:

                    @pl.when(jnp.logical_and(row + step >= 0, row + step < grid_rows))
                    def _(to_ctx=to_ctx):
                        for h in range(2):
                            send(k, to_ctx, h)

    early = [2, 2, 1]
    for stage in range(1, stages + 1):
        greeted(stage)
        if stage < stages:
            greet(stage + 1)
        for k in range(early[min(stage, len(early)) - 1]):
            send_stage(k, stage)

    for k in range(count):
        for stage in range(stages, 0, -1):
            if k >= early[min(stage, len(early)) - 1]:
                send_stage(k, stage)

    @pl.loop(0, n2)
    def _(i):
        span = my_half * n2 + i

        def find(b, at):
            return jnp.where(order_ref[b] == span, b // 2, at)

        holder[i] = lax.fori_loop(0, 2 * n2, find, jnp.int32(0))
        for slot in range(pages):
            page = jnp.int32(0)
            for p in range(pages):
                page = jnp.where(table_ref[span * pages + p] == span * pages + slot, p, page)
            source_page[i * pages + slot] = page

    def deliver(k, i, h):
        c = chunks[k]
        share = my_place - base(k, my_half)
        at = lax.rem(share, c.col_blocks) * c.share_width + h * width + c.col
        dst = out_ref.at[
            c.kv,
            :,
            pl.ds(c.unit + share // c.col_blocks * c.share_units, c.share_units),
            :,
            pl.ds(pl.multiple_of(at, LANES), 2 // c.parts * c.share_width),
        ]
        return routed[k].at[i, h], dst

    for k in range(count):

        @pl.when(taking(k))
        def _(k=k):
            pltpu.make_async_copy(shares[k], shares[k], recv1.at[k]).wait()

            @pl.loop(0, n2)
            def _(d):
                i = lax.rem(my_place + d, n2)
                c = holder[i]
                for slot in range(pages):
                    page = source_page[i * pages + slot]
                    for h in range(2):
                        if chunks[k].parts == 2:
                            routed[k][i, h, slot] = shares[k][c, h, page]
                        else:
                            routed[k][i, 0, slot, :, :, h * width : (h + 1) * width] = shares[k][
                                c, h, page
                            ]

            @pl.loop(0, n2)
            def _(d):
                i = lax.rem(my_place + d, n2)
                j = my_half * n2 + i
                for h in range(chunks[k].parts):
                    src, dst = deliver(k, i, h)

                    @pl.when(j != me)
                    def _():
                        pltpu.make_async_remote_copy(
                            src_ref=src,
                            dst_ref=dst,
                            send_sem=send2.at[k, i, h],
                            recv_sem=recv2.at[k],
                            device_id=device(j),
                            device_id_type=MESH,
                        ).start()

                    @pl.when(j == me)
                    def _():
                        pltpu.make_async_copy(src, dst, recv2.at[k]).start()

    for k in range(count):
        c = chunks[k]

        @pl.loop(0, 2 * c.takers)
        def _(d, k=k):
            half, share, j = sends(k, d)

            @pl.when(j != me)
            def _():
                src, _ = spread(k, half, share)
                pltpu.make_async_copy(src, src, send1.at[k, j]).wait()

        @pl.when(taking(k))
        def _(k=k):
            @pl.loop(1, n2)
            def _(d):
                i = lax.rem(my_place + d, n2)
                for h in range(chunks[k].parts):
                    src = routed[k].at[i, h]
                    pltpu.make_async_copy(src, src, send2.at[k, i, h]).wait()

    for k in range(count):
        both = halves[k]
        pltpu.make_async_copy(both, both, recv2.at[k]).wait()


def per_device(keys_values, span_order, page_table):
    _, tok_rows, width = keys_values.shape
    n_ctx = lax.axis_size("ctx")
    n2 = n_ctx * lax.axis_size("head") // 2
    pages = tok_rows // 2 // PAGE
    chunks = plan(n2, width)
    count = len(chunks)
    dtype = keys_values.dtype
    x = keys_values.reshape(2, 2, pages, PAGE // UNIT, UNIT, width)
    out = pl.pallas_call(
        functools.partial(kernel, n2, pages, width),
        out_shape=pltpu.VMEM((2, pages, PAGE // UNIT, UNIT, 2 * width), dtype),
        in_specs=[
            pl.BlockSpec(memory_space=pltpu.HBM),
            pl.BlockSpec(memory_space=pltpu.SMEM),
            pl.BlockSpec(memory_space=pltpu.SMEM),
        ],
        out_specs=pl.BlockSpec(memory_space=pl.ANY),
        scratch_shapes=[pltpu.VMEM((2, pages, c.units, UNIT, c.width), dtype) for c in chunks]
        + [
            pltpu.VMEM((2, c.takers, pages, c.share_units, UNIT, c.share_width), dtype)
            for c in chunks
        ]
        + [
            pltpu.VMEM((n_ctx, 2, pages, c.share_units, UNIT, c.share_width), dtype)
            for c in chunks
        ]
        + [
            pltpu.VMEM(
                (n2, c.parts, pages, c.share_units, UNIT, 2 // c.parts * c.share_width), dtype
            )
            for c in chunks
        ]
        + [
            pltpu.SMEM((n2,), jnp.int32),
            pltpu.SMEM((n2 * pages,), jnp.int32),
            pltpu.SemaphoreType.DMA((count,)),
            pltpu.SemaphoreType.DMA((count, 2 * n2)),
            pltpu.SemaphoreType.DMA((count,)),
            pltpu.SemaphoreType.DMA((count, n2, 2)),
            pltpu.SemaphoreType.DMA((count,)),
            pltpu.SemaphoreType.REGULAR((grid(n2)[2] + 1,)),
        ],
        compiler_params=pltpu.CompilerParams(collective_id=0, has_side_effects=True),
    )(x, span_order, page_table)
    return out.reshape(2, pages, PAGE, 2 * width)


def solution(mesh):
    in_specs = (P(None, ("groups", "ctx"), "head"), P("groups"), P("groups"))
    out_specs = P(None, ("groups", "ctx", "head"), None, None)
    return jax.shard_map(
        per_device, mesh=mesh, in_specs=in_specs, out_specs=out_specs, check_vma=False
    )
```

```python
import functools

import jax
import jax.numpy as jnp
from jax import lax
from jax.experimental import pallas as pl
from jax.experimental.pallas import tpu as pltpu
from jax.sharding import PartitionSpec as P

PAGE = 128
UNIT = 8
LANES = 128
REACH = 4
HEAD = [2, 2]
EARLY = (3, 3)
AHEAD = (0, 1)
LEAD = 2
FAR_FIRST = 1
MESH = pl.DeviceIdType.MESH


class Chunk:
    def __init__(self, kv, unit, units, width, takers):
        self.kv, self.unit, self.units, self.width = kv, unit, units, width
        self.takers = takers
        self.row_blocks = min(takers, units)
        self.share_units = units // self.row_blocks
        self.col_blocks = takers // self.row_blocks
        self.share_width = width // self.col_blocks
        self.parts = 1 if self.share_width == width else 2
        self.taker_rows = takers // 4

    def first_row(self, rows, half):
        return rows // 2 - self.taker_rows * (1 - half)


def plan(n2, width):
    page_units = PAGE // UNIT
    inner = min(page_units, n2 // 2)
    sizes = [inner] * (2 * page_units // inner)
    if inner >= 4 * (n2 // 2 * LANES // width):
        head = [p * inner // 4 for p in HEAD]
        sizes = head + sizes[sum(HEAD) // 4 :]
    chunks, at = [], 0
    for units in sizes:
        chunks.append(Chunk(at // page_units, at % page_units, units, width, n2 // 2))
        at += units
    return chunks


def order(count, takes):
    early, ahead = min(EARLY[takes], count), AHEAD[takes]
    steps = []
    for k in range(early):
        steps += [("X", k), ("A", k)]
    steps += [("X", k) for k in range(early, count)] + [("G", 0)]
    steps += [("B", k) for k in range(early)]
    ready = early
    for k in range(count + LEAD):
        if k < count:
            steps.append(("F", k))
            while ready < min(count, k + 1 + ahead):
                steps.append(("S", ready))
                ready += 1
        if takes and 0 <= k - LEAD < count:
            steps.append(("T", k - LEAD))
    return steps


def grid(n2):
    rows = n2 // 2
    reach = max(1, rows // REACH)
    away = rows // 2 + n2 // 8 - 1
    return rows, reach, max(-(-away // reach), -(-(rows // 2 - 1) // reach) + 1)


def kernel(n2, pages, width, x_ref, order_in, table_in, out_ref, *scratch):
    chunks = plan(n2, width)
    count = len(chunks)
    stored = scratch[0:count]
    halves = scratch[count : 2 * count]
    relays = scratch[2 * count : 3 * count]
    shares = scratch[3 * count : 4 * count]
    routed = scratch[4 * count : 5 * count]
    (order_ref, table_ref, holder, source_page, table_sem, load_sem) = scratch[5 * count : 5 * count + 6]
    (send1, recv1, send_relay, recv_relay, send2, recv2, hops) = scratch[5 * count + 6 :]

    group = lax.axis_index("groups")
    ctx = lax.axis_index("ctx")
    head = lax.axis_index("head")
    me = ctx * 2 + head
    my_half = me // n2
    rows, reach, stages = grid(n2)
    row, col = ctx // 2, lax.rem(ctx, 2)
    other = ctx + 1 - 2 * col

    def share_of(c):
        return me - c.first_row(rows, my_half) * 4

    def taking(c):
        return jnp.logical_and(share_of(c) >= 0, share_of(c) < c.takers)

    def load(k):
        c = chunks[k]
        return pltpu.make_async_copy(
            x_ref.at[c.kv, :, :, pl.ds(c.unit, c.units)], stored[k], load_sem.at[k]
        )

    def fetch(n):
        src, dst = ((order_in, order_ref), (table_in, table_ref))[n]
        return pltpu.make_async_copy(src, dst, table_sem.at[n])

    fetch(0).start()
    load(0).start()

    barrier = pltpu.get_barrier_semaphore()
    neighbours = 3 + 2 * (jnp.minimum(row, reach) + jnp.minimum(rows - 1 - row, reach))

    def greet(stage):
        sem = barrier if stage == 1 else hops.at[stage]

        def signal(to_ctx, to_head):
            pl.semaphore_signal(
                sem, inc=1, device_id=(group, to_ctx, to_head), device_id_type=MESH
            )

        for step in range(1, reach + 1):
            for sign in (-1, 1):
                to_row = row + sign * step

                @pl.when(jnp.logical_and(to_row >= 0, to_row < rows))
                def _(step=sign * step):
                    for h in range(2):
                        signal(ctx + 2 * step, h)

        signal(ctx, 1 - head)
        for h in range(2):
            signal(other, h)

    def greeted(stage):
        pl.semaphore_wait(barrier if stage == 1 else hops.at[stage], neighbours)

    greet(1)
    fetch(1).start()
    for k in range(1, count):
        load(k).start()
    fetch(0).wait()

    both_halves = (1 - my_half, my_half) if FAR_FIRST else (my_half, 1 - my_half)

    first_is_upper = (order_ref[2 * ctx] >= n2).astype(jnp.int32)

    def split(k):
        c = chunks[k]
        load(k).wait()
        for half in range(2):
            block = first_is_upper if half == 0 else 1 - first_is_upper
            for share in range(c.takers):
                unit = share // c.col_blocks * c.share_units
                at = share % c.col_blocks * c.share_width
                for page in range(pages):
                    halves[k][half * c.takers + share, page] = stored[k][
                        block, page, unit : unit + c.share_units, :, at : at + c.share_width
                    ]

    def send(k, half, share, to_ctx, to_head, dst, recv_sem):
        pltpu.make_async_remote_copy(
            src_ref=halves[k].at[half * chunks[k].takers + share],
            dst_ref=dst,
            send_sem=send1.at[k],
            recv_sem=recv_sem,
            device_id=(group, to_ctx, to_head),
            device_id_type=MESH,
        ).start()

    def cross(k):
        c = chunks[k]
        for half in both_halves:
            for t in range(c.taker_rows):
                same = row == c.first_row(rows, half) + t

                def out(dst, recv_sem, half=half, t=t):
                    for h in range(2):
                        share = t * 4 + (1 - col) * 2 + h
                        send(k, half, share, other, h, dst, recv_sem)

                @pl.when(same)
                def _(out=out):
                    out(shares[k].at[ctx, head], recv1.at[k])

                @pl.when(jnp.logical_not(same))
                def _(out=out, half=half, t=t):
                    out(relays[k].at[half * chunks[k].taker_rows + t, head], recv_relay.at[k, half])

    def straight(k, stage=None):
        c = chunks[k]
        for half in both_halves:
            for t in range(c.taker_rows):
                to_row = c.first_row(rows, half) + t
                away = jnp.abs(to_row - row)
                dst = shares[k].at[ctx, head]

                if stage is None or stage == 1:

                    @pl.when(away == 0)
                    def _(half=half, t=t, dst=dst):
                        send(k, half, t * 4 + col * 2 + 1 - head, ctx, 1 - head, dst, recv1.at[k])
                        own = halves[k].at[half * c.takers + t * 4 + col * 2 + head]
                        pltpu.make_async_copy(own, dst, recv1.at[k]).start()

                far = away > 0
                if stage is not None:
                    far = jnp.logical_and(
                        away > (stage - 1) * reach, away <= stage * reach
                    )

                @pl.when(far)
                def _(half=half, t=t, dst=dst, to_row=to_row):
                    for h in range(2):
                        send(k, half, t * 4 + col * 2 + h, to_row * 2 + col, h, dst, recv1.at[k])

    def forward(k):
        c = chunks[k]
        for half in both_halves:
            first = c.first_row(rows, half)
            top = half * c.taker_rows
            inside = jnp.logical_and(row >= first, row < first + c.taker_rows)

            def arrived(n, half=half, top=top):
                part = relays[k].at[pl.ds(top, n)]
                pltpu.make_async_copy(part, part, recv_relay.at[k, half]).wait()

            @pl.when(jnp.logical_not(inside))
            def _(arrived=arrived):
                arrived(c.taker_rows)

            if c.taker_rows > 1:

                @pl.when(inside)
                def _(arrived=arrived):
                    arrived(c.taker_rows - 1)

            for t in range(c.taker_rows):
                to_row = first + t

                @pl.when(row != to_row)
                def _(at=top + t, to_row=to_row):
                    pltpu.make_async_remote_copy(
                        src_ref=relays[k].at[at],
                        dst_ref=shares[k].at[other],
                        send_sem=send_relay.at[k],
                        recv_sem=recv1.at[k],
                        device_id=(group, to_row * 2 + col, head),
                        device_id_type=MESH,
                    ).start()

    def tables():
        fetch(1).wait()

        @pl.loop(0, n2)
        def _(i):
            span = my_half * n2 + i

            def find(b, at):
                return jnp.where(order_ref[b] == span, b // 2, at)

            holder[i] = lax.fori_loop(0, 2 * n2, find, jnp.int32(0), unroll=16)
            for slot in range(pages):
                page = jnp.int32(0)
                for p in range(pages):
                    page = jnp.where(table_ref[span * pages + p] == span * pages + slot, p, page)
                source_page[i * pages + slot] = page

    def deliver(k, i, h):
        c = chunks[k]
        my_share = share_of(c)
        at = lax.rem(my_share, c.col_blocks) * c.share_width + h * width
        dst = out_ref.at[
            c.kv,
            :,
            pl.ds(c.unit + my_share // c.col_blocks * c.share_units, c.share_units),
            :,
            pl.ds(pl.multiple_of(at, LANES), 2 // c.parts * c.share_width),
        ]
        return routed[k].at[i, h], dst

    def take(k):
        @pl.when(taking(chunks[k]))
        def _():
            pltpu.make_async_copy(shares[k], shares[k], recv1.at[k]).wait()
            start = my_half * (n2 // 2)

            @pl.loop(0, n2)
            def _(d):
                i = lax.rem(start + d, n2)
                c = holder[i]
                for slot in range(pages):
                    page = source_page[i * pages + slot]
                    for h in range(2):
                        if chunks[k].parts == 2:
                            routed[k][i, h, slot] = shares[k][c, h, page]
                        else:
                            routed[k][i, 0, slot, :, :, h * width : (h + 1) * width] = shares[k][
                                c, h, page
                            ]

            @pl.loop(0, n2)
            def _(d):
                i = lax.rem(start + d, n2)
                j = my_half * n2 + i
                for h in range(chunks[k].parts):
                    src, dst = deliver(k, i, h)

                    @pl.when(j != me)
                    def _():
                        pltpu.make_async_remote_copy(
                            src_ref=src,
                            dst_ref=dst,
                            send_sem=send2.at[k],
                            recv_sem=recv2.at[k],
                            device_id=(group, j // 2, lax.rem(j, 2)),
                            device_id_type=MESH,
                        ).start()

                    @pl.when(j == me)
                    def _():
                        pltpu.make_async_copy(src, dst, recv2.at[k]).start()

    for k in range(count):
        split(k)
    greeted(1)
    if stages > 1:
        greet(2)

    def later(k):
        for stage in range(2, stages + 1):
            straight(k, stage)

    def climb(k):
        for stage in range(2, stages + 1):
            greeted(stage)
            if stage < stages:
                greet(stage + 1)

    steps = {
        "X": cross,
        "A": lambda k: straight(k, 1),
        "B": later,
        "S": straight,
        "F": forward,
        "T": take,
        "G": climb,
    }
    inner_row = taking(chunks[0])
    tables()

    def follow(steps_in_order):
        for name, k in steps_in_order:
            steps[name](k)

    @pl.when(inner_row)
    def _():
        follow(order(count, 1))

    @pl.when(jnp.logical_not(inner_row))
    def _():
        follow(order(count, 0))

    for k in range(count):

        def sent(buf, n, sem):
            part = buf.at[pl.ds(0, n)]
            pltpu.make_async_copy(part, part, sem).wait()

        c = chunks[k]

        @pl.when(taking(c))
        def _(k=k, c=c, sent=sent):
            sent(halves[k], 2 * c.takers - 1, send1.at[k])
            sent(relays[k], 2 * c.taker_rows - 1, send_relay.at[k])
            sent(routed[k], n2 - 1, send2.at[k])

        @pl.when(jnp.logical_not(taking(c)))
        def _(k=k, c=c, sent=sent):
            sent(halves[k], 2 * c.takers, send1.at[k])
            sent(relays[k], 2 * c.taker_rows, send_relay.at[k])

    for k in range(count):
        pltpu.make_async_copy(halves[k], halves[k], recv2.at[k]).wait()


def per_device(keys_values, span_order, page_table):
    _, tok_rows, width = keys_values.shape
    n_ctx = lax.axis_size("ctx")
    n2 = n_ctx * lax.axis_size("head") // 2
    pages = tok_rows // 2 // PAGE
    chunks = plan(n2, width)
    count = len(chunks)
    stages = grid(n2)[2]
    dtype = keys_values.dtype
    x = keys_values.reshape(2, 2, pages, PAGE // UNIT, UNIT, width)

    def share(c, *lead):
        return pltpu.VMEM((*lead, pages, c.share_units, UNIT, c.share_width), dtype)

    out = pl.pallas_call(
        functools.partial(kernel, n2, pages, width),
        out_shape=pltpu.VMEM((2, pages, PAGE // UNIT, UNIT, 2 * width), dtype),
        in_specs=[
            pl.BlockSpec(memory_space=pltpu.HBM),
            pl.BlockSpec(memory_space=pltpu.HBM),
            pl.BlockSpec(memory_space=pltpu.HBM),
        ],
        out_specs=pl.BlockSpec(memory_space=pl.ANY),
        scratch_shapes=[pltpu.VMEM((2, pages, c.units, UNIT, width), dtype) for c in chunks]
        + [share(c, 2 * c.takers) for c in chunks]
        + [share(c, 2 * c.taker_rows, 2) for c in chunks]
        + [share(c, n_ctx, 2) for c in chunks]
        + [
            pltpu.VMEM(
                (n2, c.parts, pages, c.share_units, UNIT, 2 // c.parts * c.share_width), dtype
            )
            for c in chunks
        ]
        + [
            pltpu.SMEM(span_order.shape, jnp.int32),
            pltpu.SMEM(page_table.shape, jnp.int32),
            pltpu.SMEM((n2,), jnp.int32),
            pltpu.SMEM((n2 * pages,), jnp.int32),
            pltpu.SemaphoreType.DMA((2,)),
            pltpu.SemaphoreType.DMA((count,)),
            pltpu.SemaphoreType.DMA((count,)),
            pltpu.SemaphoreType.DMA((count,)),
            pltpu.SemaphoreType.DMA((count,)),
            pltpu.SemaphoreType.DMA((count, 2)),
            pltpu.SemaphoreType.DMA((count,)),
            pltpu.SemaphoreType.DMA((count,)),
            pltpu.SemaphoreType.REGULAR((stages + 1,)),
        ],
        compiler_params=pltpu.CompilerParams(collective_id=0, has_side_effects=True),
    )(x, span_order, page_table)
    return out.reshape(2, pages, PAGE, 2 * width)


def solution(mesh):
    in_specs = (P(None, ("groups", "ctx"), "head"), P("groups"), P("groups"))
    out_specs = P(None, ("groups", "ctx", "head"), None, None)
    return jax.shard_map(
        per_device, mesh=mesh, in_specs=in_specs, out_specs=out_specs, check_vma=False
    )
```

```python
import functools

import jax
import jax.numpy as jnp
from jax import lax
from jax.experimental import pallas as pl
from jax.experimental.pallas import tpu as pltpu
from jax.sharding import PartitionSpec as P

PAGE = 128
UNIT = 8
LANES = 128
REACH = 4
HEAD = [2, 2]
EARLY = (3, 3)
AHEAD = (0, 1)
LEAD = 2
FAR_FIRST = 1
MESH = pl.DeviceIdType.MESH


class Chunk:
    def __init__(self, kv, unit, units, width, takers):
        self.kv, self.unit, self.units, self.width = kv, unit, units, width
        self.takers = takers
        self.row_blocks = min(takers, units)
        self.share_units = units // self.row_blocks
        self.col_blocks = takers // self.row_blocks
        self.share_width = width // self.col_blocks
        self.parts = 1 if self.share_width == width else 2
        self.taker_rows = takers // 4

    def first_row(self, rows, half):
        return rows // 2 - self.taker_rows * (1 - half)


def plan(n2, width):
    page_units = PAGE // UNIT
    inner = min(page_units, n2 // 2)
    sizes = [inner] * (2 * page_units // inner)
    if inner >= 4 * (n2 // 2 * LANES // width):
        head = [p * inner // 4 for p in HEAD]
        sizes = head + sizes[sum(HEAD) // 4 :]
    chunks, at = [], 0
    for units in sizes:
        chunks.append(Chunk(at // page_units, at % page_units, units, width, n2 // 2))
        at += units
    return chunks


def order(count, takes):
    early, ahead = min(EARLY[takes], count), AHEAD[takes]
    steps = []
    for k in range(early):
        steps += [("X", k), ("A", k)]
    steps += [("X", k) for k in range(early, count)] + [("G", 0)]
    steps += [("B", k) for k in range(early)]
    ready = early
    for k in range(count + LEAD):
        if k < count:
            steps.append(("F", k))
            while ready < min(count, k + 1 + ahead):
                steps.append(("S", ready))
                ready += 1
        if takes and 0 <= k - LEAD < count:
            steps.append(("T", k - LEAD))
    return steps


def grid(n2):
    rows = n2 // 2
    reach = max(1, rows // REACH)
    away = rows // 2 + n2 // 8 - 1
    return rows, reach, max(-(-away // reach), -(-(rows // 2 - 1) // reach) + 1)


def kernel(n2, pages, width, x_ref, order_in, table_in, out_ref, *scratch):
    chunks = plan(n2, width)
    count = len(chunks)
    stored = scratch[0:count]
    halves = scratch[count : 2 * count]
    relays = scratch[2 * count : 3 * count]
    shares = scratch[3 * count : 4 * count]
    routed = scratch[4 * count : 5 * count]
    (order_ref, table_ref, holder, source_page, table_sem, load_sem) = scratch[5 * count : 5 * count + 6]
    (send1, recv1, send_relay, recv_relay, send2, recv2, hops) = scratch[5 * count + 6 :]

    group = lax.axis_index("groups")
    ctx = lax.axis_index("ctx")
    head = lax.axis_index("head")
    me = ctx * 2 + head
    my_half = me // n2
    rows, reach, stages = grid(n2)
    row, col = ctx // 2, lax.rem(ctx, 2)
    other = ctx + 1 - 2 * col

    def share_of(c):
        return me - c.first_row(rows, my_half) * 4

    def taking(c):
        return jnp.logical_and(share_of(c) >= 0, share_of(c) < c.takers)

    def load(k):
        c = chunks[k]
        return pltpu.make_async_copy(
            x_ref.at[c.kv, :, :, pl.ds(c.unit, c.units)], stored[k], load_sem.at[k]
        )

    def fetch(n):
        src, dst = ((order_in, order_ref), (table_in, table_ref))[n]
        return pltpu.make_async_copy(src, dst, table_sem.at[n])

    fetch(0).start()
    load(0).start()

    barrier = pltpu.get_barrier_semaphore()
    neighbours = 3 + 2 * (jnp.minimum(row, reach) + jnp.minimum(rows - 1 - row, reach))

    def greet(stage):
        sem = barrier if stage == 1 else hops.at[stage]

        def signal(to_ctx, to_head):
            pl.semaphore_signal(
                sem, inc=1, device_id=(group, to_ctx, to_head), device_id_type=MESH
            )

        for step in range(1, reach + 1):
            for sign in (-1, 1):
                to_row = row + sign * step

                @pl.when(jnp.logical_and(to_row >= 0, to_row < rows))
                def _(step=sign * step):
                    for h in range(2):
                        signal(ctx + 2 * step, h)

        signal(ctx, 1 - head)
        for h in range(2):
            signal(other, h)

    def greeted(stage):
        pl.semaphore_wait(barrier if stage == 1 else hops.at[stage], neighbours)

    greet(1)
    fetch(1).start()
    for k in range(1, count):
        load(k).start()
    fetch(0).wait()

    both_halves = (1 - my_half, my_half) if FAR_FIRST else (my_half, 1 - my_half)

    first_is_upper = (order_ref[2 * ctx] >= n2).astype(jnp.int32)

    def split(k):
        c = chunks[k]
        load(k).wait()
        for half in range(2):
            block = first_is_upper if half == 0 else 1 - first_is_upper
            for share in range(c.takers):
                unit = share // c.col_blocks * c.share_units
                at = share % c.col_blocks * c.share_width
                for page in range(pages):
                    halves[k][half * c.takers + share, page] = stored[k][
                        block, page, unit : unit + c.share_units, :, at : at + c.share_width
                    ]

    def send(k, half, share, to_ctx, to_head, dst, recv_sem):
        pltpu.make_async_remote_copy(
            src_ref=halves[k].at[half * chunks[k].takers + share],
            dst_ref=dst,
            send_sem=send1.at[k],
            recv_sem=recv_sem,
            device_id=(group, to_ctx, to_head),
            device_id_type=MESH,
        ).start()

    def cross(k):
        c = chunks[k]
        for half in both_halves:
            for t in range(c.taker_rows):
                same = row == c.first_row(rows, half) + t

                def out(dst, recv_sem, half=half, t=t):
                    for h in range(2):
                        share = t * 4 + (1 - col) * 2 + h
                        send(k, half, share, other, h, dst, recv_sem)

                @pl.when(same)
                def _(out=out):
                    out(shares[k].at[ctx, head], recv1.at[k])

                @pl.when(jnp.logical_not(same))
                def _(out=out, half=half, t=t):
                    out(relays[k].at[half * chunks[k].taker_rows + t, head], recv_relay.at[k, half])

    def straight(k, stage=None):
        c = chunks[k]
        for half in both_halves:
            for t in range(c.taker_rows):
                to_row = c.first_row(rows, half) + t
                away = jnp.abs(to_row - row)
                dst = shares[k].at[ctx, head]

                if stage is None or stage == 1:

                    @pl.when(away == 0)
                    def _(half=half, t=t, dst=dst):
                        send(k, half, t * 4 + col * 2 + 1 - head, ctx, 1 - head, dst, recv1.at[k])
                        own = halves[k].at[half * c.takers + t * 4 + col * 2 + head]
                        pltpu.make_async_copy(own, dst, recv1.at[k]).start()

                far = away > 0
                if stage is not None:
                    far = jnp.logical_and(
                        away > (stage - 1) * reach, away <= stage * reach
                    )

                @pl.when(far)
                def _(half=half, t=t, dst=dst, to_row=to_row):
                    for h in range(2):
                        send(k, half, t * 4 + col * 2 + h, to_row * 2 + col, h, dst, recv1.at[k])

    def forward(k):
        c = chunks[k]
        for half in both_halves:
            first = c.first_row(rows, half)
            top = half * c.taker_rows
            inside = jnp.logical_and(row >= first, row < first + c.taker_rows)

            def arrived(n, half=half, top=top):
                part = relays[k].at[pl.ds(top, n)]
                pltpu.make_async_copy(part, part, recv_relay.at[k, half]).wait()

            @pl.when(jnp.logical_not(inside))
            def _(arrived=arrived):
                arrived(c.taker_rows)

            if c.taker_rows > 1:

                @pl.when(inside)
                def _(arrived=arrived):
                    arrived(c.taker_rows - 1)

            for t in range(c.taker_rows):
                to_row = first + t

                @pl.when(row != to_row)
                def _(at=top + t, to_row=to_row):
                    pltpu.make_async_remote_copy(
                        src_ref=relays[k].at[at],
                        dst_ref=shares[k].at[other],
                        send_sem=send_relay.at[k],
                        recv_sem=recv1.at[k],
                        device_id=(group, to_row * 2 + col, head),
                        device_id_type=MESH,
                    ).start()

    def tables():
        fetch(1).wait()

        @pl.loop(0, n2)
        def _(i):
            span = my_half * n2 + i

            def find(b, at):
                return jnp.where(order_ref[b] == span, b // 2, at)

            holder[i] = lax.fori_loop(0, 2 * n2, find, jnp.int32(0), unroll=16)
            for slot in range(pages):
                page = jnp.int32(0)
                for p in range(pages):
                    page = jnp.where(table_ref[span * pages + p] == span * pages + slot, p, page)
                source_page[i * pages + slot] = page

    def deliver(k, i, h):
        c = chunks[k]
        my_share = share_of(c)
        at = lax.rem(my_share, c.col_blocks) * c.share_width + h * width
        dst = out_ref.at[
            c.kv,
            :,
            pl.ds(c.unit + my_share // c.col_blocks * c.share_units, c.share_units),
            :,
            pl.ds(pl.multiple_of(at, LANES), 2 // c.parts * c.share_width),
        ]
        return routed[k].at[i, h], dst

    def take(k):
        @pl.when(taking(chunks[k]))
        def _():
            pltpu.make_async_copy(shares[k], shares[k], recv1.at[k]).wait()
            start = my_half * (n2 // 2)

            @pl.loop(0, n2)
            def _(d):
                i = lax.rem(start + d, n2)
                c = holder[i]
                for slot in range(pages):
                    page = source_page[i * pages + slot]
                    for h in range(2):
                        if chunks[k].parts == 2:
                            routed[k][i, h, slot] = shares[k][c, h, page]
                        else:
                            routed[k][i, 0, slot, :, :, h * width : (h + 1) * width] = shares[k][
                                c, h, page
                            ]

            @pl.loop(0, n2)
            def _(d):
                i = lax.rem(start + d, n2)
                j = my_half * n2 + i
                for h in range(chunks[k].parts):
                    src, dst = deliver(k, i, h)

                    @pl.when(j != me)
                    def _():
                        pltpu.make_async_remote_copy(
                            src_ref=src,
                            dst_ref=dst,
                            send_sem=send2.at[k],
                            recv_sem=recv2.at[k],
                            device_id=(group, j // 2, lax.rem(j, 2)),
                            device_id_type=MESH,
                        ).start()

                    @pl.when(j == me)
                    def _():
                        pltpu.make_async_copy(src, dst, recv2.at[k]).start()

    for k in range(count):
        split(k)
    tables()
    greeted(1)
    if stages > 1:
        greet(2)

    def later(k):
        for stage in range(2, stages + 1):
            straight(k, stage)

    def climb(k):
        for stage in range(2, stages + 1):
            greeted(stage)
            if stage < stages:
                greet(stage + 1)

    steps = {
        "X": cross,
        "A": lambda k: straight(k, 1),
        "B": later,
        "S": straight,
        "F": forward,
        "T": take,
        "G": climb,
    }
    inner_row = taking(chunks[0])

    def follow(steps_in_order):
        for name, k in steps_in_order:
            steps[name](k)

    @pl.when(inner_row)
    def _():
        follow(order(count, 1))

    @pl.when(jnp.logical_not(inner_row))
    def _():
        follow(order(count, 0))

    for k in range(count):

        def sent(buf, n, sem):
            part = buf.at[pl.ds(0, n)]
            pltpu.make_async_copy(part, part, sem).wait()

        c = chunks[k]

        @pl.when(taking(c))
        def _(k=k, c=c, sent=sent):
            sent(halves[k], 2 * c.takers - 1, send1.at[k])
            sent(relays[k], 2 * c.taker_rows - 1, send_relay.at[k])
            sent(routed[k], n2 - 1, send2.at[k])

        @pl.when(jnp.logical_not(taking(c)))
        def _(k=k, c=c, sent=sent):
            sent(halves[k], 2 * c.takers, send1.at[k])
            sent(relays[k], 2 * c.taker_rows, send_relay.at[k])

    for k in range(count):
        pltpu.make_async_copy(halves[k], halves[k], recv2.at[k]).wait()


def per_device(keys_values, span_order, page_table):
    _, tok_rows, width = keys_values.shape
    n_ctx = lax.axis_size("ctx")
    n2 = n_ctx * lax.axis_size("head") // 2
    pages = tok_rows // 2 // PAGE
    chunks = plan(n2, width)
    count = len(chunks)
    stages = grid(n2)[2]
    dtype = keys_values.dtype
    x = keys_values.reshape(2, 2, pages, PAGE // UNIT, UNIT, width)

    def share(c, *lead):
        return pltpu.VMEM((*lead, pages, c.share_units, UNIT, c.share_width), dtype)

    out = pl.pallas_call(
        functools.partial(kernel, n2, pages, width),
        out_shape=pltpu.VMEM((2, pages, PAGE // UNIT, UNIT, 2 * width), dtype),
        in_specs=[
            pl.BlockSpec(memory_space=pltpu.HBM),
            pl.BlockSpec(memory_space=pltpu.HBM),
            pl.BlockSpec(memory_space=pltpu.HBM),
        ],
        out_specs=pl.BlockSpec(memory_space=pl.ANY),
        scratch_shapes=[pltpu.VMEM((2, pages, c.units, UNIT, width), dtype) for c in chunks]
        + [share(c, 2 * c.takers) for c in chunks]
        + [share(c, 2 * c.taker_rows, 2) for c in chunks]
        + [share(c, n_ctx, 2) for c in chunks]
        + [
            pltpu.VMEM(
                (n2, c.parts, pages, c.share_units, UNIT, 2 // c.parts * c.share_width), dtype
            )
            for c in chunks
        ]
        + [
            pltpu.SMEM(span_order.shape, jnp.int32),
            pltpu.SMEM(page_table.shape, jnp.int32),
            pltpu.SMEM((n2,), jnp.int32),
            pltpu.SMEM((n2 * pages,), jnp.int32),
            pltpu.SemaphoreType.DMA((2,)),
            pltpu.SemaphoreType.DMA((count,)),
            pltpu.SemaphoreType.DMA((count,)),
            pltpu.SemaphoreType.DMA((count,)),
            pltpu.SemaphoreType.DMA((count,)),
            pltpu.SemaphoreType.DMA((count, 2)),
            pltpu.SemaphoreType.DMA((count,)),
            pltpu.SemaphoreType.DMA((count,)),
            pltpu.SemaphoreType.REGULAR((stages + 1,)),
        ],
        compiler_params=pltpu.CompilerParams(collective_id=0, has_side_effects=True),
    )(x, span_order, page_table)
    return out.reshape(2, pages, PAGE, 2 * width)


def solution(mesh):
    in_specs = (P(None, ("groups", "ctx"), "head"), P("groups"), P("groups"))
    out_specs = P(None, ("groups", "ctx", "head"), None, None)
    return jax.shard_map(
        per_device, mesh=mesh, in_specs=in_specs, out_specs=out_specs, check_vma=False
    )
```
